128 devices in a mesh: shard: 32 (over y, x, core), width: 4 (over z).
Axes of the slice: x: 4, y: 4, z: 4, core: 2. Of those that a mesh axis runs over, the one named last changes fastest.
Arguments:
- w_up: bfloat16 [12288, 49152], P('shard', 'width'), may hold values from -0.109375 to 0.109375
- low_up: bfloat16 [12288, 64], P('shard'), may hold values from -0.0546875 to 0.0546875
- high_up: bfloat16 [64, 49152], P(None, 'width'), may hold values from -0.75 to 0.75
- norm_train: float32 [12288], P(('shard', 'width')), may hold values from 0.25 to 1.75
- norm_step: float32 [12288], P(('shard', 'width')), may hold values from -0.3 to 0.3
Outputs:
- serve_up: bfloat16 [12288, 49152], P(None, ('width', 'shard'))
- scale_up: float32 [49152], P(('width', 'shard'))
- serve_norm: bfloat16 [12288], replicated
The draws below stay inside these ranges and needn't reach their ends.
All inputs are finite; a program needn't handle non-finite values. Where the reference program divides by a largest or mean magnitude, that divisor is 1e-20 or more.
Results may differ from the reference program's by a relative error of at most 0.001.
Values may be sent and summed in bfloat16 or wider, within the bound.
A program may use at most 128 MiB of HBM per device.

```python
import jax
import jax.numpy as jnp

D_MODEL = 12288
D_INNER = 49152
RANK = 64


def raised(drawn, own_key, source, target, blocks, factor):
    def block_of(dim):
        return (jnp.arange(drawn.shape[dim]) // (drawn.shape[dim] // blocks)).reshape((-1,) + (1,) * (drawn.ndim - 1 - dim))

    one_side = jax.random.permutation(own_key, blocks)[block_of(target)]
    far = (block_of(target) + blocks // 2) % blocks
    return jnp.where((block_of(source) == one_side) | (block_of(source) == far), factor * drawn, drawn)


def block_levels(rng, extent, shards, smallest, high):
    def one(dim, parts):
        draws = jax.random.uniform(jax.random.fold_in(jax.random.fold_in(rng, 6), dim), (parts,), jnp.float32, smallest / len(shards), high / len(shards))
        return jnp.repeat(jnp.exp(draws), extent[dim] // parts).reshape((-1,) + (1,) * (len(extent) - dim - 1))

    gain = one(*shards[0])
    for cut in shards[1:]:
        gain = gain * one(*cut)
    return gain


def gaussian(rng, dims, width, reach, split=(), held_as=jnp.bfloat16):
    entries = width * jax.random.normal(rng, dims, jnp.float32)
    if split:
        entries = entries * block_levels(rng, dims, split, -0.22, 0.18)
    return jnp.clip(entries, -reach, reach).astype(held_as)


def heavy_noise(rng, extent, deviation, bound, cuts, heavy, held_as=jnp.bfloat16):
    result = deviation * jax.random.normal(rng, extent, jnp.float32)
    if cuts:
        result = result * block_levels(rng, extent, cuts, -0.22, 0.18)
    return jnp.clip(raised(result, jax.random.fold_in(rng, 3), *heavy), -bound, bound).astype(held_as)


def setup_inputs(seed: int = 0) -> dict:
    key_of = jax.random.split(jax.random.key(seed), 6)
    w_up = heavy_noise(key_of[0], (D_MODEL, D_INNER), D_MODEL ** -0.5, 0.109375, ((0, 32), (1, 4)), (0, 1, 32, 2.75))
    low_up = gaussian(key_of[1], (D_MODEL, RANK), D_MODEL ** -0.5, 0.0546875, ((0, 32),))
    high_up = gaussian(key_of[2], (RANK, D_INNER), RANK ** -0.5, 0.75, ((1, 4),))
    norm_train = jnp.clip(1.0 + 0.15 * jax.random.normal(key_of[3], (D_MODEL,), jnp.float32), 0.25, 1.75)
    norm_step = jnp.clip(jax.random.uniform(key_of[4], (D_MODEL,), jnp.float32, -0.3, 0.3) * block_levels(key_of[4], (D_MODEL,), ((0, 128),), -0.4, 0.0), -0.3, 0.3)
    return dict(w_up=w_up, low_up=low_up, high_up=high_up, norm_train=norm_train, norm_step=norm_step)


mix_rate = 0.5


def reference(w_up, low_up, high_up, norm_train, norm_step):
    fresh_up = w_up.astype(jnp.float32) + mix_rate * jnp.dot(low_up, high_up, preferred_element_type=jnp.float32)
    scale_up = jnp.sum(jnp.abs(fresh_up), axis=0) / D_MODEL
    serve_up = (fresh_up / scale_up).astype(jnp.bfloat16)
    serve_norm = (norm_train + norm_step).astype(jnp.bfloat16)
    return serve_up, scale_up, serve_norm
```

```python
import functools

import jax
import jax.numpy as jnp
from jax import lax
from jax.experimental import pallas as pl
from jax.experimental.pallas import tpu as pltpu
from jax.sharding import Mesh
from jax.sharding import PartitionSpec as P

D_MODEL = 12288
RANK = 64
SIDE = 4
CORES = 2
CHIPS = SIDE * SIDE
GROUP = CHIPS * CORES
ROWS = D_MODEL // GROUP
COLS = 384
PIECE = RANK // SIDE
NORM = 96
STEP = 128
SHARD = ("shard_0", "shard_1", "shard_2")
SHARD_WIDTH = ("shard_0", "shard_1", "shard_2", "width")
WIDTH_SHARD = ("width", "shard_0", "shard_1", "shard_2")
MESH = pl.DeviceIdType.MESH

mix_rate = 0.5


def hops(*pairs):
    def wrapped(v):
        return tuple(q % SIDE for q in v) if isinstance(v, tuple) else (v % SIDE,) * 2

    return [(wrapped(dy), wrapped(dx), dc) for dc in range(CORES) for dy, dx in pairs]


STAGES = [
    hops((1, 1), (-1, -1)) + [((0, 0), (0, 0), 1)],
    hops((1, -1), (-1, 1)),
    hops((0, 2), (2, 0)),
    hops((2, 2)),
    hops((1, 2), (-1, 2), (1, 0), (-1, 0)),
    hops(((2, 0), 1), ((2, 0), -1)),
    hops(((0, 2), 1), ((0, 2), -1)),
]
FIRST = [sum(len(s) for s in STAGES[:k]) for k in range(len(STAGES) + 1)]
AHEAD = 2


def by_core(core, value):
    return value[0] if value[0] == value[1] else jnp.where(core == 0, value[0], value[1])


def exchange(
    w, low, high, train, step,
    rows, lows, own_high, scale, norms,
    norm_own, norm_z, norm_mid, total,
    send, recv, low_send, low_recv, low_zsend, low_zrecv, nz_send, nz_recv, n_send, n_recv, local,
):
    y, x, core = (lax.axis_index(a) for a in SHARD)
    z = lax.axis_index("width")
    chip = y * SIDE + x
    me = chip * CORES + core

    def at(dy, dx, dc):
        return lax.rem(y + dy, SIDE), lax.rem(x + dx, SIDE), lax.rem(core + dc, CORES)

    def device(ty, tx, tc, tz=None):
        return {"shard_0": ty, "shard_1": tx, "shard_2": tc, "width": z if tz is None else tz}

    plane = [(dy, dx, dc) for dy in range(SIDE) for dx in range(SIDE) for dc in range(CORES)][1:]
    column = [(dz, dc) for dz in range(SIDE) for dc in range(CORES)][1:]

    get_high = pltpu.make_async_copy(
        high.at[:, pl.ds(pl.multiple_of(me * COLS, 128), COLS)], own_high, local.at[0]
    )
    get_high.start()
    get_rows = pltpu.make_async_copy(
        w.at[:, pl.ds(pl.multiple_of(me * COLS, 128), COLS)],
        rows.at[pl.ds(pl.multiple_of(me * ROWS, ROWS), ROWS), :],
        local.at[1],
    )
    get_rows.start()
    get_low = pltpu.make_async_copy(
        low.at[pl.ds(pl.multiple_of(z * PIECE, PIECE), PIECE), :], lows.at[z, core, chip], local.at[2]
    )
    get_low.start()
    norm_own[...] = jnp.zeros_like(norm_own)
    norm_own[0, :, 0:NORM] = (train[...] + step[...]).astype(jnp.bfloat16).astype(jnp.float32)

    barrier = pltpu.get_barrier_semaphore()
    for dy, dx, dc in plane:
        pl.semaphore_signal(barrier, inc=1, device_id=device(*at(dy, dx, dc)), device_id_type=MESH)
    for dz, dc in column[1:]:
        to = device(y, x, lax.rem(core + dc, CORES), lax.rem(z + dz, SIDE))
        pl.semaphore_signal(barrier, inc=1, device_id=to, device_id_type=MESH)
    pl.semaphore_wait(barrier, len(plane) + len(column) - 1)

    low_copies = []
    for k, (dy, dx, dc) in enumerate([h for h in plane if h[2] == 0]):
        low_copies.append(
            pltpu.make_async_remote_copy(
                src_ref=low.at[pl.ds(pl.multiple_of(z * PIECE, PIECE), PIECE), :],
                dst_ref=lows.at[z, core, chip],
                send_sem=low_send.at[k],
                recv_sem=low_recv.at[k],
                device_id=device(*at(dy, dx, 0)),
                device_id_type=MESH,
            )
        )
    for c in low_copies:
        c.start()
    nz_copies = [
        pltpu.make_async_remote_copy(
            src_ref=norm_own.at[0],
            dst_ref=norm_z.at[z],
            send_sem=nz_send.at[dz - 1],
            recv_sem=nz_recv.at[dz - 1],
            device_id=device(y, x, core, lax.rem(z + dz, SIDE)),
            device_id_type=MESH,
        )
        for dz in range(1, SIDE)
    ]
    for c in nz_copies:
        c.start()
    norm_z[z] = norm_own[0]

    def row_copy(i, hop):
        ty, tx, tc = at(by_core(core, hop[0]), by_core(core, hop[1]), hop[2])
        to = (ty * SIDE + tx) * CORES + tc
        return pltpu.make_async_remote_copy(
            src_ref=w.at[:, pl.ds(pl.multiple_of(to * COLS, 128), COLS)],
            dst_ref=rows.at[pl.ds(pl.multiple_of(me * ROWS, ROWS), ROWS), :],
            send_sem=send.at[i],
            recv_sem=recv.at[i],
            device_id=device(ty, tx, tc),
            device_id_type=MESH,
        )

    copies = [[row_copy(FIRST[k] + i, hop) for i, hop in enumerate(s)] for k, s in enumerate(STAGES)]

    def start(k):
        if k >= AHEAD:
            for c in copies[k - AHEAD]:
                c.wait_send()
        for c in copies[k]:
            c.start()

    def add_block(source_chip, source_core):
        base = (source_chip * CORES + source_core) * ROWS
        for r in range(0, ROWS, STEP):
            left = lows[:, source_core, source_chip, :, r : r + STEP].reshape(RANK, STEP)
            change = lax.dot_general(
                left, own_high[...], (((0,), (0,)), ((), ())), preferred_element_type=jnp.float32
            )
            fresh = rows[pl.ds(pl.multiple_of(base + r, STEP), STEP), :].astype(jnp.float32) + change
            total[...] += jnp.abs(fresh).reshape(STEP // 8, 8, COLS).sum(axis=0)

    def take(k):
        stage = STAGES[k]

        def one(i, carry):
            def pick(values):
                out = values[0]
                for j in range(1, len(values)):
                    out = jnp.where(i == j, values[j], out)
                return out

            dc = pick([h[2] for h in stage])
            source_core = lax.rem(core + dc, CORES)
            dy = jnp.where(source_core == 0, pick([h[0][0] for h in stage]), pick([h[0][1] for h in stage]))
            dx = jnp.where(source_core == 0, pick([h[1][0] for h in stage]), pick([h[1][1] for h in stage]))
            source_chip = lax.rem(y + SIDE - dy, SIDE) * SIDE + lax.rem(x + SIDE - dx, SIDE)
            base = (source_chip * CORES + source_core) * ROWS
            landed = rows.at[pl.ds(pl.multiple_of(base, ROWS), ROWS), :]
            pltpu.make_async_copy(landed, landed, recv.at[FIRST[k] + i]).wait()
            add_block(source_chip, source_core)
            return carry

        lax.fori_loop(0, len(stage), one, 0)

    start(0)
    start(1)

    get_low.wait()
    for c in low_copies:
        c.wait_recv()
    low_zcopies = []
    for k, (dz, dc) in enumerate(column):
        low_zcopies.append(
            pltpu.make_async_remote_copy(
                src_ref=lows.at[z, core],
                dst_ref=lows.at[z, core],
                send_sem=low_zsend.at[k],
                recv_sem=low_zrecv.at[k],
                device_id=device(y, x, lax.rem(core + dc, CORES), lax.rem(z + dz, SIDE)),
                device_id_type=MESH,
            )
        )
    for c in low_zcopies:
        c.start()

    for c in nz_copies:
        c.wait_recv()
    lane = lax.broadcasted_iota(jnp.int32, (1, 128), 1)
    second = pltpu.roll(norm_z[1], NORM, 1)
    third = pltpu.roll(norm_z[2], 64, 1)
    fourth = pltpu.roll(norm_z[3], 32, 1)
    norm_mid[0] = jnp.where(lane < NORM, norm_z[0], second)
    norm_mid[1] = jnp.where(lane < 64, second, third)
    norm_mid[2] = jnp.where(lane < 32, third, fourth)
    for j in range(3):
        norms[me * 3 + j] = norm_mid[j]
    own_high[...] = own_high_half(get_high, own_high)
    total[...] = jnp.zeros_like(total)

    start(2)
    norm_copies = [
        pltpu.make_async_remote_copy(
            src_ref=norm_mid,
            dst_ref=norms.at[pl.ds(me * 3, 3)],
            send_sem=n_send.at[k],
            recv_sem=n_recv.at[k],
            device_id=device(*at(dy, dx, dc)),
            device_id_type=MESH,
        )
        for k, (dy, dx, dc) in enumerate(plane)
    ]
    for c in norm_copies:
        c.start()
    start(3)
    for c in low_zcopies:
        c.wait_recv()
    get_rows.wait()
    add_block(chip, core)
    take(0)
    start(4)
    take(1)
    start(5)
    take(2)
    start(6)
    for k in range(3, len(STAGES)):
        take(k)
    for k in range(len(STAGES) - AHEAD, len(STAGES)):
        for c in copies[k]:
            c.wait_send()
    for c in low_copies + low_zcopies + nz_copies + norm_copies:
        c.wait_send()
    for c in norm_copies:
        c.wait_recv()
    scale[...] = total[...].sum(axis=0, keepdims=True) / D_MODEL


def own_high_half(copy, own_high):
    copy.wait()
    return (own_high[...].astype(jnp.float32) * mix_rate).astype(jnp.bfloat16)


SLOTS = 4


def finish(rows, lows, own_high, scale, norms, serve, scale_out, norm_out, slots, sems):
    scale_out[...] = scale[...]
    norm_out[...] = norms[...].reshape(D_MODEL // 128, 128).astype(jnp.bfloat16)
    inverse = 1.0 / scale[...]

    def put(n, slot):
        to = serve.at[pl.ds(pl.multiple_of(n * ROWS, ROWS), ROWS), :]
        return pltpu.make_async_copy(slots.at[slot], to, sems.at[slot])

    def one(n, carry):
        slot = lax.rem(n, SLOTS)

        @pl.when(n >= SLOTS)
        def _():
            put(n - SLOTS, slot).wait()

        source_chip, source_core = n // CORES, lax.rem(n, CORES)
        for r in range(0, ROWS, STEP):
            left = lows[:, source_core, source_chip, :, r : r + STEP].reshape(RANK, STEP)
            change = lax.dot_general(
                left, own_high[...], (((0,), (0,)), ((), ())), preferred_element_type=jnp.float32
            )
            fresh = rows[pl.ds(pl.multiple_of(n * ROWS + r, STEP), STEP), :].astype(jnp.float32) + change
            slots[slot, r : r + STEP, :] = (fresh * inverse).astype(jnp.bfloat16)
        put(n, slot).start()
        return carry

    lax.fori_loop(0, GROUP, one, 0)
    for n in range(GROUP - SLOTS, GROUP):
        put(n, n % SLOTS).wait()


def per_device(w_up, low_up, high_up, norm_train, norm_step):
    dma = pltpu.SemaphoreType.DMA
    anywhere = pl.BlockSpec(memory_space=pl.ANY)
    vmem = pl.BlockSpec(memory_space=pltpu.VMEM)
    chips = CHIPS - 1
    column = SIDE * CORES - 1
    total = FIRST[-1]
    gathered = pl.pallas_call(
        exchange,
        out_shape=(
            pltpu.VMEM((D_MODEL, COLS), jnp.bfloat16),
            pltpu.VMEM((SIDE, CORES, CHIPS, PIECE, ROWS), jnp.bfloat16),
            pltpu.VMEM((RANK, COLS), jnp.bfloat16),
            pltpu.VMEM((1, COLS), jnp.float32),
            pltpu.VMEM((D_MODEL // 128, 1, 128), jnp.float32),
        ),
        in_specs=[anywhere, anywhere, anywhere, vmem, vmem],
        out_specs=(vmem,) * 5,
        scratch_shapes=[
            pltpu.VMEM((1, 1, 128), jnp.float32),
            pltpu.VMEM((SIDE, 1, 128), jnp.float32),
            pltpu.VMEM((3, 1, 128), jnp.float32),
            pltpu.VMEM((8, COLS), jnp.float32),
            dma((total,)),
            dma((total,)),
            dma((chips,)),
            dma((chips,)),
            dma((column,)),
            dma((column,)),
            dma((SIDE - 1,)),
            dma((SIDE - 1,)),
            dma((GROUP - 1,)),
            dma((GROUP - 1,)),
            dma((3,)),
        ],
        compiler_params=pltpu.CompilerParams(
            collective_id=0, has_side_effects=True, vmem_limit_bytes=8 * 2**20
        ),
        name="exchange",
    )(w_up, low_up.T, high_up, norm_train.reshape(1, NORM), norm_step.reshape(1, NORM))
    serve_up, scale_up, serve_norm = pl.pallas_call(
        finish,
        out_shape=(
            jax.ShapeDtypeStruct((D_MODEL, COLS), jnp.bfloat16),
            jax.ShapeDtypeStruct((1, COLS), jnp.float32),
            jax.ShapeDtypeStruct((D_MODEL // 128, 128), jnp.bfloat16),
        ),
        in_specs=[vmem] * 5,
        out_specs=(anywhere, vmem, vmem),
        scratch_shapes=[pltpu.VMEM((SLOTS, ROWS, COLS), jnp.bfloat16), dma((SLOTS,))],
        compiler_params=pltpu.CompilerParams(vmem_limit_bytes=16 * 2**20),
        name="finish",
    )(*gathered)
    return serve_up, scale_up.reshape(COLS), serve_norm.reshape(D_MODEL)


def solution(mesh):
    torus = Mesh(
        mesh.devices.reshape(SIDE, SIDE, CORES, mesh.shape["width"]),
        ("shard_0", "shard_1", "shard_2", "width"),
    )
    in_specs = (P(SHARD, "width"), P(SHARD, None), P(None, "width"), P(SHARD_WIDTH), P(SHARD_WIDTH))
    out_specs = (P(None, WIDTH_SHARD), P(WIDTH_SHARD), P())
    return jax.shard_map(
        per_device, mesh=torus, in_specs=in_specs, out_specs=out_specs, check_vma=False
    )
```

```python
import functools

import jax
import jax.numpy as jnp
from jax import lax
from jax.experimental import pallas as pl
from jax.experimental.pallas import tpu as pltpu
from jax.sharding import Mesh
from jax.sharding import PartitionSpec as P

D_MODEL = 12288
RANK = 64
SIDE = 4
CORES = 2
CHIPS = SIDE * SIDE
GROUP = CHIPS * CORES
ROWS = D_MODEL // GROUP
COLS = 384
PIECE = RANK // SIDE
NORM = 96
STEP = 128
SHARD = ("shard_0", "shard_1", "shard_2")
SHARD_WIDTH = ("shard_0", "shard_1", "shard_2", "width")
WIDTH_SHARD = ("width", "shard_0", "shard_1", "shard_2")
MESH = pl.DeviceIdType.MESH

mix_rate = 0.5


def hops(*pairs):
    def wrapped(v):
        return tuple(q % SIDE for q in v) if isinstance(v, tuple) else (v % SIDE,) * 2

    return [(wrapped(dy), wrapped(dx), dc) for dc in range(CORES) for dy, dx in pairs]


STAGES = [
    hops((1, 1), (-1, -1)) + [((0, 0), (0, 0), 1)],
    hops((1, -1), (-1, 1)),
    hops((0, 2), (2, 0)),
    hops((2, 2)),
    hops((1, 2), (-1, 2), (1, 0), (-1, 0)),
    hops(((2, 0), 1), ((2, 0), -1)),
    hops(((0, 2), 1), ((0, 2), -1)),
]
FIRST = [sum(len(s) for s in STAGES[:k]) for k in range(len(STAGES) + 1)]
AHEAD = 2


def by_core(core, value):
    return value[0] if value[0] == value[1] else jnp.where(core == 0, value[0], value[1])


def exchange(
    w, low, high, train, step,
    fresh_out, scale, norms,
    rows, lows, own_high, norm_in, norm_own, norm_z, norm_mid, total,
    send, recv, low_send, low_recv, low_zsend, low_zrecv, nz_send, nz_recv, n_send, n_recv, local,
):
    y, x, core = (lax.axis_index(a) for a in SHARD)
    z = lax.axis_index("width")
    chip = y * SIDE + x
    me = chip * CORES + core

    def at(dy, dx, dc):
        return lax.rem(y + dy, SIDE), lax.rem(x + dx, SIDE), lax.rem(core + dc, CORES)

    def device(ty, tx, tc, tz=None):
        return {"shard_0": ty, "shard_1": tx, "shard_2": tc, "width": z if tz is None else tz}

    plane = [(dy, dx, dc) for dy in range(SIDE) for dx in range(SIDE) for dc in range(CORES)][1:]
    column = [(dz, dc) for dz in range(SIDE) for dc in range(CORES)][1:]

    get_high = pltpu.make_async_copy(
        high.at[:, pl.ds(pl.multiple_of(me * COLS, 128), COLS)], own_high, local.at[0]
    )
    get_high.start()
    get_rows = pltpu.make_async_copy(
        w.at[:, pl.ds(pl.multiple_of(me * COLS, 128), COLS)],
        rows.at[pl.ds(pl.multiple_of(me * ROWS, ROWS), ROWS), :],
        local.at[1],
    )
    get_rows.start()
    get_low = pltpu.make_async_copy(
        low.at[pl.ds(pl.multiple_of(z * PIECE, PIECE), PIECE), :], lows.at[z, core, chip], local.at[2]
    )
    get_low.start()
    get_norms = [
        pltpu.make_async_copy(part, norm_in.at[k], local.at[3 + k]) for k, part in enumerate((train, step))
    ]
    for c in get_norms:
        c.start()
    norm_own[...] = jnp.zeros_like(norm_own)

    barrier = pltpu.get_barrier_semaphore()
    for dy, dx, dc in plane:
        pl.semaphore_signal(barrier, inc=1, device_id=device(*at(dy, dx, dc)), device_id_type=MESH)
    for dz, dc in column[1:]:
        to = device(y, x, lax.rem(core + dc, CORES), lax.rem(z + dz, SIDE))
        pl.semaphore_signal(barrier, inc=1, device_id=to, device_id_type=MESH)
    pl.semaphore_wait(barrier, len(plane) + len(column) - 1)

    low_copies = []
    for k, (dy, dx, dc) in enumerate([h for h in plane if h[2] == 0]):
        low_copies.append(
            pltpu.make_async_remote_copy(
                src_ref=low.at[pl.ds(pl.multiple_of(z * PIECE, PIECE), PIECE), :],
                dst_ref=lows.at[z, core, chip],
                send_sem=low_send.at[k],
                recv_sem=low_recv.at[k],
                device_id=device(*at(dy, dx, 0)),
                device_id_type=MESH,
            )
        )
    for c in low_copies:
        c.start()
    for c in get_norms:
        c.wait()
    norm_own[0, :, 0:NORM] = (norm_in[0] + norm_in[1]).astype(jnp.bfloat16).astype(jnp.float32)
    nz_copies = [
        pltpu.make_async_remote_copy(
            src_ref=norm_own.at[0],
            dst_ref=norm_z.at[z],
            send_sem=nz_send.at[dz - 1],
            recv_sem=nz_recv.at[dz - 1],
            device_id=device(y, x, core, lax.rem(z + dz, SIDE)),
            device_id_type=MESH,
        )
        for dz in range(1, SIDE)
    ]

    def row_copy(i, hop):
        ty, tx, tc = at(by_core(core, hop[0]), by_core(core, hop[1]), hop[2])
        to = (ty * SIDE + tx) * CORES + tc
        return pltpu.make_async_remote_copy(
            src_ref=w.at[:, pl.ds(pl.multiple_of(to * COLS, 128), COLS)],
            dst_ref=rows.at[pl.ds(pl.multiple_of(me * ROWS, ROWS), ROWS), :],
            send_sem=send.at[i],
            recv_sem=recv.at[i],
            device_id=device(ty, tx, tc),
            device_id_type=MESH,
        )

    copies = [[row_copy(FIRST[k] + i, hop) for i, hop in enumerate(s)] for k, s in enumerate(STAGES)]

    def start(k):
        if k >= AHEAD:
            for c in copies[k - AHEAD]:
                c.wait_send()
        for c in copies[k]:
            c.start()

    def add_block(source_chip, source_core):
        base = (source_chip * CORES + source_core) * ROWS
        for r in range(0, ROWS, STEP):
            left = lows[:, source_core, source_chip, :, r : r + STEP].reshape(RANK, STEP)
            change = lax.dot_general(
                left, own_high[...], (((0,), (0,)), ((), ())), preferred_element_type=jnp.float32
            )
            fresh = rows[pl.ds(pl.multiple_of(base + r, STEP), STEP), :].astype(jnp.float32) + change
            fresh_out[pl.ds(pl.multiple_of(base + r, STEP), STEP), :] = fresh
            total[...] += jnp.abs(fresh).reshape(STEP // 8, 8, COLS).sum(axis=0)

    def take(k):
        stage = STAGES[k]

        def one(i, carry):
            def pick(values):
                out = values[0]
                for j in range(1, len(values)):
                    out = jnp.where(i == j, values[j], out)
                return out

            dc = pick([h[2] for h in stage])
            source_core = lax.rem(core + dc, CORES)
            dy = jnp.where(source_core == 0, pick([h[0][0] for h in stage]), pick([h[0][1] for h in stage]))
            dx = jnp.where(source_core == 0, pick([h[1][0] for h in stage]), pick([h[1][1] for h in stage]))
            source_chip = lax.rem(y + SIDE - dy, SIDE) * SIDE + lax.rem(x + SIDE - dx, SIDE)
            base = (source_chip * CORES + source_core) * ROWS
            landed = rows.at[pl.ds(pl.multiple_of(base, ROWS), ROWS), :]
            pltpu.make_async_copy(landed, landed, recv.at[FIRST[k] + i]).wait()
            add_block(source_chip, source_core)
            return carry

        lax.fori_loop(0, len(stage), one, 0)

    start(0)
    start(1)

    for c in nz_copies:
        c.start()
    norm_z[z] = norm_own[0]
    get_low.wait()
    for c in low_copies:
        c.wait_recv()
    low_zcopies = []
    for k, (dz, dc) in enumerate(column):
        low_zcopies.append(
            pltpu.make_async_remote_copy(
                src_ref=lows.at[z, core],
                dst_ref=lows.at[z, core],
                send_sem=low_zsend.at[k],
                recv_sem=low_zrecv.at[k],
                device_id=device(y, x, lax.rem(core + dc, CORES), lax.rem(z + dz, SIDE)),
                device_id_type=MESH,
            )
        )
    for c in low_zcopies:
        c.start()

    for c in nz_copies:
        c.wait_recv()
    lane = lax.broadcasted_iota(jnp.int32, (1, 128), 1)
    second = pltpu.roll(norm_z[1], NORM, 1)
    third = pltpu.roll(norm_z[2], 64, 1)
    fourth = pltpu.roll(norm_z[3], 32, 1)
    norm_mid[0] = jnp.where(lane < NORM, norm_z[0], second)
    norm_mid[1] = jnp.where(lane < 64, second, third)
    norm_mid[2] = jnp.where(lane < 32, third, fourth)
    for j in range(3):
        norms[me * 3 + j] = norm_mid[j]
    own_high[...] = own_high_half(get_high, own_high)
    total[...] = jnp.zeros_like(total)

    start(2)
    norm_copies = [
        pltpu.make_async_remote_copy(
            src_ref=norm_mid,
            dst_ref=norms.at[pl.ds(me * 3, 3)],
            send_sem=n_send.at[k],
            recv_sem=n_recv.at[k],
            device_id=device(*at(dy, dx, dc)),
            device_id_type=MESH,
        )
        for k, (dy, dx, dc) in enumerate(plane)
    ]
    for c in norm_copies:
        c.start()
    start(3)
    for c in low_zcopies:
        c.wait_recv()
    get_rows.wait()
    add_block(chip, core)
    take(0)
    start(4)
    take(1)
    start(5)
    take(2)
    start(6)
    for k in range(3, len(STAGES)):
        take(k)
    for k in range(len(STAGES) - AHEAD, len(STAGES)):
        for c in copies[k]:
            c.wait_send()
    for c in low_copies + low_zcopies + nz_copies + norm_copies:
        c.wait_send()
    for c in norm_copies:
        c.wait_recv()
    scale[...] = total[...].sum(axis=0, keepdims=True) / D_MODEL


def own_high_half(copy, own_high):
    copy.wait()
    return (own_high[...].astype(jnp.float32) * mix_rate).astype(jnp.bfloat16)


SLOTS = 4


def finish(fresh, scale, norms, serve, scale_out, norm_out, slots, sems):
    scale_out[...] = scale[...].reshape(COLS)
    norm_out[...] = norms[...].reshape(D_MODEL // 128, 128).astype(jnp.bfloat16)
    inverse = jnp.broadcast_to(1.0 / scale[...], (8, COLS))

    def put(n, slot):
        to = serve.at[pl.ds(pl.multiple_of(n * ROWS, ROWS), ROWS), :]
        return pltpu.make_async_copy(slots.at[slot], to, sems.at[slot])

    def one(n, carry):
        slot = lax.rem(n, SLOTS)

        @pl.when(n >= SLOTS)
        def _():
            put(n - SLOTS, slot).wait()

        part = fresh[pl.ds(pl.multiple_of(n * ROWS, ROWS), ROWS), :].reshape(ROWS // 8, 8, COLS)
        slots[slot] = (part * inverse).reshape(ROWS, COLS).astype(jnp.bfloat16)
        put(n, slot).start()
        return carry

    lax.fori_loop(0, GROUP, one, 0)
    for n in range(GROUP - SLOTS, GROUP):
        put(n, n % SLOTS).wait()


def per_device(w_up, low_up, high_up, norm_train, norm_step):
    dma = pltpu.SemaphoreType.DMA
    vmem = pl.BlockSpec(memory_space=pltpu.VMEM)
    chips = CHIPS - 1
    column = SIDE * CORES - 1
    total = FIRST[-1]
    operands = (w_up, low_up.T, high_up, norm_train.reshape(1, NORM), norm_step.reshape(1, NORM))
    gathered = pl.pallas_call(
        exchange,
        out_shape=(
            pltpu.VMEM((D_MODEL, COLS), jnp.float32),
            pltpu.VMEM((1, COLS), jnp.float32),
            pltpu.VMEM((D_MODEL // 128, 1, 128), jnp.float32),
        ),
        in_specs=[pl.BlockSpec(memory_space=pltpu.HBM)] * 5,
        out_specs=(vmem,) * 3,
        scratch_shapes=[
            pltpu.VMEM((D_MODEL, COLS), jnp.bfloat16),
            pltpu.VMEM((SIDE, CORES, CHIPS, PIECE, ROWS), jnp.bfloat16),
            pltpu.VMEM((RANK, COLS), jnp.bfloat16),
            pltpu.VMEM((2, 1, NORM), jnp.float32),
            pltpu.VMEM((1, 1, 128), jnp.float32),
            pltpu.VMEM((SIDE, 1, 128), jnp.float32),
            pltpu.VMEM((3, 1, 128), jnp.float32),
            pltpu.VMEM((8, COLS), jnp.float32),
            dma((total,)),
            dma((total,)),
            dma((chips,)),
            dma((chips,)),
            dma((column,)),
            dma((column,)),
            dma((SIDE - 1,)),
            dma((SIDE - 1,)),
            dma((GROUP - 1,)),
            dma((GROUP - 1,)),
            dma((5,)),
        ],
        compiler_params=pltpu.CompilerParams(
            collective_id=0, has_side_effects=True, vmem_limit_bytes=20 * 2**20
        ),
        name="exchange",
    )(*(pltpu.with_memory_space_constraint(a, pltpu.HBM) for a in operands))
    serve_up, scale_up, serve_norm = pl.pallas_call(
        finish,
        out_shape=(
            jax.ShapeDtypeStruct((D_MODEL, COLS), jnp.bfloat16),
            jax.ShapeDtypeStruct((COLS,), jnp.float32),
            jax.ShapeDtypeStruct((D_MODEL // 128, 128), jnp.bfloat16),
        ),
        in_specs=[vmem] * 3,
        out_specs=(pl.BlockSpec(memory_space=pltpu.HBM), vmem, vmem),
        scratch_shapes=[pltpu.VMEM((SLOTS, ROWS, COLS), jnp.bfloat16), dma((SLOTS,))],
        compiler_params=pltpu.CompilerParams(vmem_limit_bytes=6 * 2**20),
        name="finish",
    )(*gathered)
    return serve_up, scale_up, serve_norm.reshape(D_MODEL)


def solution(mesh):
    torus = Mesh(
        mesh.devices.reshape(SIDE, SIDE, CORES, mesh.shape["width"]),
        ("shard_0", "shard_1", "shard_2", "width"),
    )
    in_specs = (P(SHARD, "width"), P(SHARD, None), P(None, "width"), P(SHARD_WIDTH), P(SHARD_WIDTH))
    out_specs = (P(None, WIDTH_SHARD), P(WIDTH_SHARD), P())
    return jax.shard_map(
        per_device, mesh=torus, in_specs=in_specs, out_specs=out_specs, check_vma=False
    )
```

```python
import functools

import jax
import jax.numpy as jnp
from jax import lax
from jax.experimental import pallas as pl
from jax.experimental.pallas import tpu as pltpu
from jax.sharding import Mesh
from jax.sharding import PartitionSpec as P

D_MODEL = 12288
RANK = 64
SIDE = 4
CORES = 2
CHIPS = SIDE * SIDE
GROUP = CHIPS * CORES
ROWS = D_MODEL // GROUP
COLS = 384
PIECE = RANK // SIDE
NORM = 96
STEP = 128
SHARD = ("shard_0", "shard_1", "shard_2")
SHARD_WIDTH = ("shard_0", "shard_1", "shard_2", "width")
WIDTH_SHARD = ("width", "shard_0", "shard_1", "shard_2")
MESH = pl.DeviceIdType.MESH

mix_rate = 0.5


def hops(*pairs):
    def wrapped(v):
        return tuple(q % SIDE for q in v) if isinstance(v, tuple) else (v % SIDE,) * 2

    return [(wrapped(dy), wrapped(dx), dc) for dc in range(CORES) for dy, dx in pairs]


STAGES = [
    hops((1, 1), (-1, -1)) + [((0, 0), (0, 0), 1)],
    hops((1, -1), (-1, 1)),
    hops((0, 2), (2, 0)),
    hops((2, 2)),
    hops((1, 2), (-1, 2), (1, 0), (-1, 0)),
    hops(((2, 0), 1), ((2, 0), -1)),
    hops(((0, 2), 1), ((0, 2), -1)),
]
FIRST = [sum(len(s) for s in STAGES[:k]) for k in range(len(STAGES) + 1)]
AHEAD = 2


def by_core(core, value):
    return value[0] if value[0] == value[1] else jnp.where(core == 0, value[0], value[1])


def exchange(
    w, low, high, train, step,
    fresh_out, scale, norms,
    rows, lows, own_high, norm_in, norm_own, norm_z, norm_mid, total,
    send, recv, low_send, low_recv, low_zsend, low_zrecv, nz_send, nz_recv, n_send, n_recv, local,
):
    y, x, core = (lax.axis_index(a) for a in SHARD)
    z = lax.axis_index("width")
    chip = y * SIDE + x
    me = chip * CORES + core

    def at(dy, dx, dc):
        return lax.rem(y + dy, SIDE), lax.rem(x + dx, SIDE), lax.rem(core + dc, CORES)

    def device(ty, tx, tc, tz=None):
        return {"shard_0": ty, "shard_1": tx, "shard_2": tc, "width": z if tz is None else tz}

    plane = [(dy, dx, dc) for dy in range(SIDE) for dx in range(SIDE) for dc in range(CORES)][1:]
    column = [(dz, dc) for dz in range(SIDE) for dc in range(CORES)][1:]

    get_high = pltpu.make_async_copy(
        high.at[:, pl.ds(pl.multiple_of(me * COLS, 128), COLS)], own_high, local.at[0]
    )
    get_high.start()
    get_rows = pltpu.make_async_copy(
        w.at[:, pl.ds(pl.multiple_of(me * COLS, 128), COLS)],
        rows.at[pl.ds(pl.multiple_of(me * ROWS, ROWS), ROWS), :],
        local.at[1],
    )
    get_rows.start()
    get_low = pltpu.make_async_copy(
        low.at[pl.ds(pl.multiple_of(z * PIECE, PIECE), PIECE), :], lows.at[z, core, chip], local.at[2]
    )
    get_low.start()
    get_norms = [
        pltpu.make_async_copy(part, norm_in.at[k], local.at[3 + k]) for k, part in enumerate((train, step))
    ]
    for c in get_norms:
        c.start()
    norm_own[...] = jnp.zeros_like(norm_own)

    barrier = pltpu.get_barrier_semaphore()
    for dy, dx, dc in plane:
        pl.semaphore_signal(barrier, inc=1, device_id=device(*at(dy, dx, dc)), device_id_type=MESH)
    for dz, dc in column[1:]:
        to = device(y, x, lax.rem(core + dc, CORES), lax.rem(z + dz, SIDE))
        pl.semaphore_signal(barrier, inc=1, device_id=to, device_id_type=MESH)
    pl.semaphore_wait(barrier, len(plane) + len(column) - 1)

    low_copies = []
    for k, (dy, dx, dc) in enumerate([h for h in plane if h[2] == 0]):
        low_copies.append(
            pltpu.make_async_remote_copy(
                src_ref=low.at[pl.ds(pl.multiple_of(z * PIECE, PIECE), PIECE), :],
                dst_ref=lows.at[z, core, chip],
                send_sem=low_send.at[k],
                recv_sem=low_recv.at[k],
                device_id=device(*at(dy, dx, 0)),
                device_id_type=MESH,
            )
        )
    for c in low_copies:
        c.start()
    for c in get_norms:
        c.wait()
    norm_own[0, :, 0:NORM] = (norm_in[0] + norm_in[1]).astype(jnp.bfloat16).astype(jnp.float32)
    nz_copies = [
        pltpu.make_async_remote_copy(
            src_ref=norm_own.at[0],
            dst_ref=norm_z.at[z],
            send_sem=nz_send.at[dz - 1],
            recv_sem=nz_recv.at[dz - 1],
            device_id=device(y, x, core, lax.rem(z + dz, SIDE)),
            device_id_type=MESH,
        )
        for dz in range(1, SIDE)
    ]

    def row_copy(i, hop):
        ty, tx, tc = at(by_core(core, hop[0]), by_core(core, hop[1]), hop[2])
        to = (ty * SIDE + tx) * CORES + tc
        return pltpu.make_async_remote_copy(
            src_ref=w.at[:, pl.ds(pl.multiple_of(to * COLS, 128), COLS)],
            dst_ref=rows.at[pl.ds(pl.multiple_of(me * ROWS, ROWS), ROWS), :],
            send_sem=send.at[i],
            recv_sem=recv.at[i],
            device_id=device(ty, tx, tc),
            device_id_type=MESH,
        )

    copies = [[row_copy(FIRST[k] + i, hop) for i, hop in enumerate(s)] for k, s in enumerate(STAGES)]

    def start(k):
        if k >= AHEAD:
            for c in copies[k - AHEAD]:
                c.wait_send()
        for c in copies[k]:
            c.start()

    def add_block(source_chip, source_core):
        base = (source_chip * CORES + source_core) * ROWS
        for r in range(0, ROWS, STEP):
            left = lows[:, source_core, source_chip, :, r : r + STEP].reshape(RANK, STEP)
            change = lax.dot_general(
                left, own_high[...], (((0,), (0,)), ((), ())), preferred_element_type=jnp.float32
            )
            fresh = rows[pl.ds(pl.multiple_of(base + r, STEP), STEP), :].astype(jnp.float32) + change
            fresh_out[pl.ds(pl.multiple_of(base + r, STEP), STEP), :] = fresh
            total[...] += jnp.abs(fresh).reshape(STEP // 8, 8, COLS).sum(axis=0)

    def take(k):
        stage = STAGES[k]

        def one(i, carry):
            def pick(values):
                out = values[0]
                for j in range(1, len(values)):
                    out = jnp.where(i == j, values[j], out)
                return out

            dc = pick([h[2] for h in stage])
            source_core = lax.rem(core + dc, CORES)
            dy = jnp.where(source_core == 0, pick([h[0][0] for h in stage]), pick([h[0][1] for h in stage]))
            dx = jnp.where(source_core == 0, pick([h[1][0] for h in stage]), pick([h[1][1] for h in stage]))
            source_chip = lax.rem(y + SIDE - dy, SIDE) * SIDE + lax.rem(x + SIDE - dx, SIDE)
            base = (source_chip * CORES + source_core) * ROWS
            landed = rows.at[pl.ds(pl.multiple_of(base, ROWS), ROWS), :]
            pltpu.make_async_copy(landed, landed, recv.at[FIRST[k] + i]).wait()
            add_block(source_chip, source_core)
            return carry

        lax.fori_loop(0, len(stage), one, 0)

    start(0)
    start(1)

    for c in nz_copies:
        c.start()
    norm_z[z] = norm_own[0]
    get_low.wait()
    for c in low_copies:
        c.wait_recv()
    low_zcopies = []
    for k, (dz, dc) in enumerate(column):
        low_zcopies.append(
            pltpu.make_async_remote_copy(
                src_ref=lows.at[z, core],
                dst_ref=lows.at[z, core],
                send_sem=low_zsend.at[k],
                recv_sem=low_zrecv.at[k],
                device_id=device(y, x, lax.rem(core + dc, CORES), lax.rem(z + dz, SIDE)),
                device_id_type=MESH,
            )
        )
    for c in low_zcopies:
        c.start()

    for c in nz_copies:
        c.wait_recv()
    lane = lax.broadcasted_iota(jnp.int32, (1, 128), 1)
    second = pltpu.roll(norm_z[1], NORM, 1)
    third = pltpu.roll(norm_z[2], 64, 1)
    fourth = pltpu.roll(norm_z[3], 32, 1)
    norm_mid[0] = jnp.where(lane < NORM, norm_z[0], second)
    norm_mid[1] = jnp.where(lane < 64, second, third)
    norm_mid[2] = jnp.where(lane < 32, third, fourth)
    for j in range(3):
        norms[me * 3 + j] = norm_mid[j]
    own_high[...] = own_high_half(get_high, own_high)
    total[...] = jnp.zeros_like(total)

    start(2)
    norm_copies = [
        pltpu.make_async_remote_copy(
            src_ref=norm_mid,
            dst_ref=norms.at[pl.ds(me * 3, 3)],
            send_sem=n_send.at[k],
            recv_sem=n_recv.at[k],
            device_id=device(*at(dy, dx, dc)),
            device_id_type=MESH,
        )
        for k, (dy, dx, dc) in enumerate(plane)
    ]
    for c in norm_copies:
        c.start()
    start(3)
    for c in low_zcopies:
        c.wait_recv()
    get_rows.wait()
    add_block(chip, core)
    for k in range(4, len(STAGES)):
        take(k - 4)
        start(k)
    for k in range(len(STAGES) - 4, len(STAGES)):
        take(k)
    for k in range(len(STAGES) - AHEAD, len(STAGES)):
        for c in copies[k]:
            c.wait_send()
    for c in low_copies + low_zcopies + nz_copies + norm_copies:
        c.wait_send()
    for c in norm_copies:
        c.wait_recv()
    scale[...] = total[...].sum(axis=0, keepdims=True) / D_MODEL


def own_high_half(copy, own_high):
    copy.wait()
    return (own_high[...].astype(jnp.float32) * mix_rate).astype(jnp.bfloat16)


SLOTS = 8


def finish(fresh, scale, norms, serve, scale_out, norm_out, slots, sems):
    inverse = jnp.broadcast_to(1.0 / scale[...], (8, COLS))

    def put(n, slot):
        to = serve.at[pl.ds(pl.multiple_of(n * ROWS, ROWS), ROWS), :]
        return pltpu.make_async_copy(slots.at[slot], to, sems.at[slot])

    def one(n, carry):
        slot = lax.rem(n, SLOTS)

        @pl.when(n >= SLOTS)
        def _():
            put(n - SLOTS, slot).wait()

        part = fresh[pl.ds(pl.multiple_of(n * ROWS, ROWS), ROWS), :].reshape(ROWS // 8, 8, COLS)
        slots[slot] = (part * inverse).reshape(ROWS, COLS).astype(jnp.bfloat16)
        put(n, slot).start()
        return carry

    lax.fori_loop(0, GROUP, one, 0)
    scale_out[...] = scale[...].reshape(COLS)
    norm_out[...] = norms[...].reshape(D_MODEL // 128, 128).astype(jnp.bfloat16)
    for n in range(GROUP - SLOTS, GROUP):
        put(n, n % SLOTS).wait()


def per_device(w_up, low_up, high_up, norm_train, norm_step):
    dma = pltpu.SemaphoreType.DMA
    vmem = pl.BlockSpec(memory_space=pltpu.VMEM)
    chips = CHIPS - 1
    column = SIDE * CORES - 1
    total = FIRST[-1]
    operands = (w_up, low_up.T, high_up, norm_train.reshape(1, NORM), norm_step.reshape(1, NORM))
    gathered = pl.pallas_call(
        exchange,
        out_shape=(
            pltpu.VMEM((D_MODEL, COLS), jnp.float32),
            pltpu.VMEM((1, COLS), jnp.float32),
            pltpu.VMEM((D_MODEL // 128, 1, 128), jnp.float32),
        ),
        in_specs=[pl.BlockSpec(memory_space=pltpu.HBM)] * 5,
        out_specs=(vmem,) * 3,
        scratch_shapes=[
            pltpu.VMEM((D_MODEL, COLS), jnp.bfloat16),
            pltpu.VMEM((SIDE, CORES, CHIPS, PIECE, ROWS), jnp.bfloat16),
            pltpu.VMEM((RANK, COLS), jnp.bfloat16),
            pltpu.VMEM((2, 1, NORM), jnp.float32),
            pltpu.VMEM((1, 1, 128), jnp.float32),
            pltpu.VMEM((SIDE, 1, 128), jnp.float32),
            pltpu.VMEM((3, 1, 128), jnp.float32),
            pltpu.VMEM((8, COLS), jnp.float32),
            dma((total,)),
            dma((total,)),
            dma((chips,)),
            dma((chips,)),
            dma((column,)),
            dma((column,)),
            dma((SIDE - 1,)),
            dma((SIDE - 1,)),
            dma((GROUP - 1,)),
            dma((GROUP - 1,)),
            dma((5,)),
        ],
        compiler_params=pltpu.CompilerParams(
            collective_id=0, has_side_effects=True, vmem_limit_bytes=20 * 2**20
        ),
        name="exchange",
    )(*(pltpu.with_memory_space_constraint(a, pltpu.HBM) for a in operands))
    serve_up, scale_up, serve_norm = pl.pallas_call(
        finish,
        out_shape=(
            jax.ShapeDtypeStruct((D_MODEL, COLS), jnp.bfloat16),
            jax.ShapeDtypeStruct((COLS,), jnp.float32),
            jax.ShapeDtypeStruct((D_MODEL // 128, 128), jnp.bfloat16),
        ),
        in_specs=[vmem] * 3,
        out_specs=(pl.BlockSpec(memory_space=pltpu.HBM), vmem, vmem),
        scratch_shapes=[pltpu.VMEM((SLOTS, ROWS, COLS), jnp.bfloat16), dma((SLOTS,))],
        compiler_params=pltpu.CompilerParams(vmem_limit_bytes=6 * 2**20),
        name="finish",
    )(*gathered)
    return serve_up, scale_up, serve_norm.reshape(D_MODEL)


def solution(mesh):
    torus = Mesh(
        mesh.devices.reshape(SIDE, SIDE, CORES, mesh.shape["width"]),
        ("shard_0", "shard_1", "shard_2", "width"),
    )
    in_specs = (P(SHARD, "width"), P(SHARD, None), P(None, "width"), P(SHARD_WIDTH), P(SHARD_WIDTH))
    out_specs = (P(None, WIDTH_SHARD), P(WIDTH_SHARD), P())
    return jax.shard_map(
        per_device, mesh=torus, in_specs=in_specs, out_specs=out_specs, check_vma=False
    )
```

```python
import functools

import jax
import jax.numpy as jnp
from jax import lax
from jax.experimental import pallas as pl
from jax.experimental.pallas import tpu as pltpu
from jax.sharding import Mesh
from jax.sharding import PartitionSpec as P

D_MODEL = 12288
RANK = 64
SIDE = 4
CORES = 2
CHIPS = SIDE * SIDE
GROUP = CHIPS * CORES
ROWS = D_MODEL // GROUP
COLS = 384
PIECE = RANK // SIDE
NORM = 96
STEP = 128
SHARD = ("shard_0", "shard_1", "shard_2")
SHARD_WIDTH = ("shard_0", "shard_1", "shard_2", "width")
WIDTH_SHARD = ("width", "shard_0", "shard_1", "shard_2")
MESH = pl.DeviceIdType.MESH

mix_rate = 0.5


def hops(*pairs):
    def wrapped(v):
        return tuple(q % SIDE for q in v) if isinstance(v, tuple) else (v % SIDE,) * 2

    return [(wrapped(dy), wrapped(dx), dc) for dc in range(CORES) for dy, dx in pairs]


STAGES = [
    hops((1, 1), (-1, -1)) + [((0, 0), (0, 0), 1)],
    hops((1, -1), (-1, 1)),
    hops((0, 2), (2, 0)),
    hops((2, 2)),
    hops((1, 2), (-1, 2), (1, 0), (-1, 0)),
    hops(((2, 0), 1), ((2, 0), -1)),
    hops(((0, 2), 1), ((0, 2), -1)),
]
FIRST = [sum(len(s) for s in STAGES[:k]) for k in range(len(STAGES) + 1)]
AHEAD = 2


def by_core(core, value):
    return value[0] if value[0] == value[1] else jnp.where(core == 0, value[0], value[1])


def exchange(
    w, low, high, train, step,
    fresh_out, scale, norms,
    rows, lows, own_high, norm_in, norm_own, norm_z, norm_mid, total,
    send, recv, low_send, low_recv, low_zsend, low_zrecv, nz_send, nz_recv, n_send, n_recv, local,
):
    y, x, core = (lax.axis_index(a) for a in SHARD)
    z = lax.axis_index("width")
    chip = y * SIDE + x
    me = chip * CORES + core
    slow, fast = jnp.where(core == 0, y, x), jnp.where(core == 0, x, y)

    def at(dy, dx, dc):
        return lax.rem(y + dy, SIDE), lax.rem(x + dx, SIDE), lax.rem(core + dc, CORES)

    def device(ty, tx, tc, tz=None):
        return {"shard_0": ty, "shard_1": tx, "shard_2": tc, "width": z if tz is None else tz}

    plane = [(dy, dx, dc) for dy in range(SIDE) for dx in range(SIDE) for dc in range(CORES)][1:]
    column = [(dz, dc) for dz in range(SIDE) for dc in range(CORES)][1:]

    barrier = pltpu.get_barrier_semaphore()
    for dy, dx, dc in plane:
        pl.semaphore_signal(barrier, inc=1, device_id=device(*at(dy, dx, dc)), device_id_type=MESH)
    for dz, dc in column[1:]:
        to = device(y, x, lax.rem(core + dc, CORES), lax.rem(z + dz, SIDE))
        pl.semaphore_signal(barrier, inc=1, device_id=to, device_id_type=MESH)
    get_high = pltpu.make_async_copy(
        high.at[:, pl.ds(pl.multiple_of(me * COLS, 128), COLS)], own_high, local.at[0]
    )
    get_high.start()
    get_rows = pltpu.make_async_copy(
        w.at[:, pl.ds(pl.multiple_of(me * COLS, 128), COLS)],
        rows.at[pl.ds(pl.multiple_of(me * ROWS, ROWS), ROWS), :],
        local.at[1],
    )
    get_rows.start()
    get_low = pltpu.make_async_copy(
        low.at[pl.ds(pl.multiple_of(z * PIECE, PIECE), PIECE), :], lows.at[z, core, slow, fast], local.at[2]
    )
    get_low.start()
    get_norms = [
        pltpu.make_async_copy(part, norm_in.at[k], local.at[3 + k]) for k, part in enumerate((train, step))
    ]
    for c in get_norms:
        c.start()
    norm_own[...] = jnp.zeros_like(norm_own)

    pl.semaphore_wait(barrier, len(plane) + len(column) - 1)

    def low_copy(k, t, source, target):
        along, across = lax.rem(fast + t, SIDE), lax.rem(slow + t, SIDE)
        if k == 0:
            ty, tx = jnp.where(core == 0, y, along), jnp.where(core == 0, along, x)
        else:
            ty, tx = jnp.where(core == 0, across, y), jnp.where(core == 0, x, across)
        return pltpu.make_async_remote_copy(
            src_ref=source,
            dst_ref=target,
            send_sem=low_send.at[k * (SIDE - 1) + t - 1],
            recv_sem=low_recv.at[k * (SIDE - 1) + t - 1],
            device_id=device(ty, tx, core),
            device_id_type=MESH,
        )

    own_low = low.at[pl.ds(pl.multiple_of(z * PIECE, PIECE), PIECE), :]
    own_line = lows.at[z, core, slow]
    low_first = [low_copy(0, t, own_low, lows.at[z, core, slow, fast]) for t in range(1, SIDE)]
    low_then = [low_copy(1, t, own_line, own_line) for t in range(1, SIDE)]
    low_copies = low_first + low_then
    for c in low_first:
        c.start()
    nz_copies = [
        pltpu.make_async_remote_copy(
            src_ref=norm_own.at[0],
            dst_ref=norm_z.at[z],
            send_sem=nz_send.at[dz - 1],
            recv_sem=nz_recv.at[dz - 1],
            device_id=device(y, x, core, lax.rem(z + dz, SIDE)),
            device_id_type=MESH,
        )
        for dz in range(1, SIDE)
    ]

    def row_copy(i, hop):
        ty, tx, tc = at(by_core(core, hop[0]), by_core(core, hop[1]), hop[2])
        to = (ty * SIDE + tx) * CORES + tc
        return pltpu.make_async_remote_copy(
            src_ref=w.at[:, pl.ds(pl.multiple_of(to * COLS, 128), COLS)],
            dst_ref=rows.at[pl.ds(pl.multiple_of(me * ROWS, ROWS), ROWS), :],
            send_sem=send.at[i],
            recv_sem=recv.at[i],
            device_id=device(ty, tx, tc),
            device_id_type=MESH,
        )

    copies = [[row_copy(FIRST[k] + i, hop) for i, hop in enumerate(s)] for k, s in enumerate(STAGES)]

    def start(k):
        if k >= AHEAD:
            for c in copies[k - AHEAD]:
                c.wait_send()
        for c in copies[k]:
            c.start()

    def add_block(source_chip, source_core):
        base = (source_chip * CORES + source_core) * ROWS
        sy, sx = source_chip // SIDE, lax.rem(source_chip, SIDE)
        line, place = jnp.where(source_core == 0, sy, sx), jnp.where(source_core == 0, sx, sy)
        for r in range(0, ROWS, STEP):
            left = lows[:, source_core, line, place, :, r : r + STEP].reshape(RANK, STEP)
            change = lax.dot_general(
                left, own_high[...], (((0,), (0,)), ((), ())), preferred_element_type=jnp.float32
            )
            fresh = rows[pl.ds(pl.multiple_of(base + r, STEP), STEP), :].astype(jnp.float32) + change
            fresh_out[pl.ds(pl.multiple_of(base + r, STEP), STEP), :] = fresh
            total[...] += jnp.abs(fresh).reshape(STEP // 8, 8, COLS).sum(axis=0)

    def take(k):
        stage = STAGES[k]

        def one(i, carry):
            def pick(values):
                out = values[0]
                for j in range(1, len(values)):
                    out = jnp.where(i == j, values[j], out)
                return out

            dc = pick([h[2] for h in stage])
            source_core = lax.rem(core + dc, CORES)
            dy = jnp.where(source_core == 0, pick([h[0][0] for h in stage]), pick([h[0][1] for h in stage]))
            dx = jnp.where(source_core == 0, pick([h[1][0] for h in stage]), pick([h[1][1] for h in stage]))
            source_chip = lax.rem(y + SIDE - dy, SIDE) * SIDE + lax.rem(x + SIDE - dx, SIDE)
            base = (source_chip * CORES + source_core) * ROWS
            landed = rows.at[pl.ds(pl.multiple_of(base, ROWS), ROWS), :]
            pltpu.make_async_copy(landed, landed, recv.at[FIRST[k] + i]).wait()
            add_block(source_chip, source_core)
            return carry

        lax.fori_loop(0, len(stage), one, 0)

    start(0)
    start(1)

    for c in get_norms:
        c.wait()
    norm_own[0, :, 0:NORM] = (norm_in[0] + norm_in[1]).astype(jnp.bfloat16).astype(jnp.float32)
    for c in nz_copies:
        c.start()
    norm_z[z] = norm_own[0]
    for c in nz_copies:
        c.wait_recv()
    lane = lax.broadcasted_iota(jnp.int32, (1, 128), 1)
    second = pltpu.roll(norm_z[1], NORM, 1)
    third = pltpu.roll(norm_z[2], 64, 1)
    fourth = pltpu.roll(norm_z[3], 32, 1)
    norm_mid[0] = jnp.where(lane < NORM, norm_z[0], second)
    norm_mid[1] = jnp.where(lane < 64, second, third)
    norm_mid[2] = jnp.where(lane < 32, third, fourth)
    for j in range(3):
        norms[me * 3 + j] = norm_mid[j]
    own_high[...] = own_high_half(get_high, own_high)
    total[...] = jnp.zeros_like(total)

    start(2)
    norm_copies = [
        pltpu.make_async_remote_copy(
            src_ref=norm_mid,
            dst_ref=norms.at[pl.ds(me * 3, 3)],
            send_sem=n_send.at[k],
            recv_sem=n_recv.at[k],
            device_id=device(*at(dy, dx, dc)),
            device_id_type=MESH,
        )
        for k, (dy, dx, dc) in enumerate(plane)
    ]
    low_zcopies = []
    for k, (dz, dc) in enumerate(column):
        low_zcopies.append(
            pltpu.make_async_remote_copy(
                src_ref=lows.at[z, core],
                dst_ref=lows.at[z, core],
                send_sem=low_zsend.at[k],
                recv_sem=low_zrecv.at[k],
                device_id=device(y, x, lax.rem(core + dc, CORES), lax.rem(z + dz, SIDE)),
                device_id_type=MESH,
            )
        )
    start(3)
    get_low.wait()
    for c in low_first:
        c.wait_recv()
    for c in low_then:
        c.start()
    start(4)
    start(5)
    for c in norm_copies:
        c.start()
    for c in low_then:
        c.wait_recv()
    for c in low_zcopies:
        c.start()
    start(6)
    for c in low_zcopies:
        c.wait_recv()
    get_rows.wait()
    add_block(chip, core)
    take(0)
    take(1)
    take(2)
    take(3)
    take(4)
    take(5)
    take(6)
    for k in range(len(STAGES) - AHEAD, len(STAGES)):
        for c in copies[k]:
            c.wait_send()
    for c in low_copies + low_zcopies + nz_copies + norm_copies:
        c.wait_send()
    for c in norm_copies:
        c.wait_recv()
    scale[...] = total[...].sum(axis=0, keepdims=True) / D_MODEL


def own_high_half(copy, own_high):
    copy.wait()
    return (own_high[...].astype(jnp.float32) * mix_rate).astype(jnp.bfloat16)


SLOTS = 8


def finish(fresh, scale, norms, serve, scale_out, norm_out, slots, sems, scale_row, norm_rows, small):
    inverse = jnp.broadcast_to(1.0 / scale[...], (8, COLS))

    def put(n, slot):
        to = serve.at[pl.ds(pl.multiple_of(n * ROWS, ROWS), ROWS), :]
        return pltpu.make_async_copy(slots.at[slot], to, sems.at[slot])

    def one(n, carry):
        slot = lax.rem(n, SLOTS)

        @pl.when(n >= SLOTS)
        def _():
            put(n - SLOTS, slot).wait()

        part = fresh[pl.ds(pl.multiple_of(n * ROWS, ROWS), ROWS), :].reshape(ROWS // 8, 8, COLS)
        slots[slot] = (part * inverse).reshape(ROWS, COLS).astype(jnp.bfloat16)
        put(n, slot).start()
        return carry

    lax.fori_loop(0, GROUP - SLOTS, one, 0)
    scale_row[...] = scale[...].reshape(COLS)
    norm_rows[...] = norms[...].reshape(D_MODEL // 128, 128).astype(jnp.bfloat16)
    rest = [
        pltpu.make_async_copy(scale_row, scale_out, small.at[0]),
        pltpu.make_async_copy(norm_rows, norm_out, small.at[1]),
    ]
    for c in rest:
        c.start()
    lax.fori_loop(GROUP - SLOTS, GROUP, one, 0)
    for c in rest:
        c.wait()
    for n in range(GROUP - SLOTS, GROUP):
        put(n, n % SLOTS).wait()


def per_device(w_up, low_up, high_up, norm_train, norm_step):
    dma = pltpu.SemaphoreType.DMA
    vmem = pl.BlockSpec(memory_space=pltpu.VMEM)
    column = SIDE * CORES - 1
    total = FIRST[-1]
    operands = (w_up, low_up.T, high_up, norm_train.reshape(1, NORM), norm_step.reshape(1, NORM))
    gathered = pl.pallas_call(
        exchange,
        out_shape=(
            pltpu.VMEM((D_MODEL, COLS), jnp.float32),
            pltpu.VMEM((1, COLS), jnp.float32),
            pltpu.VMEM((D_MODEL // 128, 1, 128), jnp.float32),
        ),
        in_specs=[pl.BlockSpec(memory_space=pltpu.HBM)] * 5,
        out_specs=(vmem,) * 3,
        scratch_shapes=[
            pltpu.VMEM((D_MODEL, COLS), jnp.bfloat16),
            pltpu.VMEM((SIDE, CORES, SIDE, SIDE, PIECE, ROWS), jnp.bfloat16),
            pltpu.VMEM((RANK, COLS), jnp.bfloat16),
            pltpu.VMEM((2, 1, NORM), jnp.float32),
            pltpu.VMEM((1, 1, 128), jnp.float32),
            pltpu.VMEM((SIDE, 1, 128), jnp.float32),
            pltpu.VMEM((3, 1, 128), jnp.float32),
            pltpu.VMEM((8, COLS), jnp.float32),
            dma((total,)),
            dma((total,)),
            dma((2 * (SIDE - 1),)),
            dma((2 * (SIDE - 1),)),
            dma((column,)),
            dma((column,)),
            dma((SIDE - 1,)),
            dma((SIDE - 1,)),
            dma((GROUP - 1,)),
            dma((GROUP - 1,)),
            dma((5,)),
        ],
        compiler_params=pltpu.CompilerParams(
            collective_id=0, has_side_effects=True, vmem_limit_bytes=20 * 2**20
        ),
        name="exchange",
    )(*(pltpu.with_memory_space_constraint(a, pltpu.HBM) for a in operands))
    serve_up, scale_up, serve_norm = pl.pallas_call(
        finish,
        out_shape=(
            jax.ShapeDtypeStruct((D_MODEL, COLS), jnp.bfloat16),
            jax.ShapeDtypeStruct((COLS,), jnp.float32),
            jax.ShapeDtypeStruct((D_MODEL // 128, 128), jnp.bfloat16),
        ),
        in_specs=[vmem] * 3,
        out_specs=(pl.BlockSpec(memory_space=pltpu.HBM),) * 3,
        scratch_shapes=[
            pltpu.VMEM((SLOTS, ROWS, COLS), jnp.bfloat16),
            dma((SLOTS,)),
            pltpu.VMEM((COLS,), jnp.float32),
            pltpu.VMEM((D_MODEL // 128, 128), jnp.bfloat16),
            dma((2,)),
        ],
        compiler_params=pltpu.CompilerParams(vmem_limit_bytes=6 * 2**20),
        name="finish",
    )(*gathered)
    return serve_up, scale_up, serve_norm.reshape(D_MODEL)


def solution(mesh):
    torus = Mesh(
        mesh.devices.reshape(SIDE, SIDE, CORES, mesh.shape["width"]),
        ("shard_0", "shard_1", "shard_2", "width"),
    )
    in_specs = (P(SHARD, "width"), P(SHARD, None), P(None, "width"), P(SHARD_WIDTH), P(SHARD_WIDTH))
    out_specs = (P(None, WIDTH_SHARD), P(WIDTH_SHARD), P())
    return jax.shard_map(
        per_device, mesh=torus, in_specs=in_specs, out_specs=out_specs, check_vma=False
    )
```

```python
import functools

import jax
import jax.numpy as jnp
from jax import lax
from jax.experimental import pallas as pl
from jax.experimental.pallas import tpu as pltpu
from jax.sharding import Mesh
from jax.sharding import PartitionSpec as P

D_MODEL = 12288
RANK = 64
SIDE = 4
CORES = 2
CHIPS = SIDE * SIDE
GROUP = CHIPS * CORES
ROWS = D_MODEL // GROUP
COLS = 384
PIECE = RANK // SIDE
NORM = 96
STEP = 128
SHARD = ("shard_0", "shard_1", "shard_2")
SHARD_WIDTH = ("shard_0", "shard_1", "shard_2", "width")
WIDTH_SHARD = ("width", "shard_0", "shard_1", "shard_2")
MESH = pl.DeviceIdType.MESH

mix_rate = 0.5


def hops(*pairs):
    def wrapped(v):
        return tuple(q % SIDE for q in v) if isinstance(v, tuple) else (v % SIDE,) * 2

    return [(wrapped(dy), wrapped(dx), dc) for dc in range(CORES) for dy, dx in pairs]


STAGES = [
    hops((1, 1), (-1, -1)) + [((0, 0), (0, 0), 1)],
    hops((1, -1), (-1, 1)),
    hops((2, 2)),
    hops((0, 2), (2, 0)),
    hops((1, 2), (-1, 2), (1, 0), (-1, 0)),
    hops(((2, 0), 1), ((2, 0), -1)),
    hops(((0, 2), 1), ((0, 2), -1)),
]
FIRST = [sum(len(s) for s in STAGES[:k]) for k in range(len(STAGES) + 1)]
AHEAD = 2


def by_core(core, value):
    return value[0] if value[0] == value[1] else jnp.where(core == 0, value[0], value[1])


def exchange(
    w, low, high, train, step,
    fresh_out, scale, norms,
    rows, lows, own_high, norm_in, norm_own, norm_z, norm_mid, norm_all, total,
    send, recv, low_send, low_recv, low_zsend, low_zrecv, nz_send, nz_recv, n_send, n_recv, local,
):
    y, x, core = (lax.axis_index(a) for a in SHARD)
    z = lax.axis_index("width")
    chip = y * SIDE + x
    me = chip * CORES + core
    slow, fast = jnp.where(core == 0, y, x), jnp.where(core == 0, x, y)

    def at(dy, dx, dc):
        return lax.rem(y + dy, SIDE), lax.rem(x + dx, SIDE), lax.rem(core + dc, CORES)

    def device(ty, tx, tc, tz=None):
        return {"shard_0": ty, "shard_1": tx, "shard_2": tc, "width": z if tz is None else tz}

    plane = [(dy, dx, dc) for dy in range(SIDE) for dx in range(SIDE) for dc in range(CORES)][1:]
    column = [(dz, dc) for dz in range(SIDE) for dc in range(CORES)][1:]

    barrier = pltpu.get_barrier_semaphore()
    for dy, dx, dc in plane:
        pl.semaphore_signal(barrier, inc=1, device_id=device(*at(dy, dx, dc)), device_id_type=MESH)
    for dz, dc in column[1:]:
        to = device(y, x, lax.rem(core + dc, CORES), lax.rem(z + dz, SIDE))
        pl.semaphore_signal(barrier, inc=1, device_id=to, device_id_type=MESH)
    get_high = pltpu.make_async_copy(
        high.at[:, pl.ds(pl.multiple_of(me * COLS, 128), COLS)], own_high, local.at[0]
    )
    get_high.start()
    get_rows = pltpu.make_async_copy(
        w.at[:, pl.ds(pl.multiple_of(me * COLS, 128), COLS)],
        rows.at[pl.ds(pl.multiple_of(me * ROWS, ROWS), ROWS), :],
        local.at[1],
    )
    get_rows.start()
    get_low = pltpu.make_async_copy(
        low.at[pl.ds(pl.multiple_of(z * PIECE, PIECE), PIECE), :], lows.at[z, core, slow, fast], local.at[2]
    )
    get_low.start()
    get_norms = [
        pltpu.make_async_copy(part, norm_in.at[k], local.at[3 + k]) for k, part in enumerate((train, step))
    ]
    for c in get_norms:
        c.start()
    norm_own[...] = jnp.zeros_like(norm_own)

    pl.semaphore_wait(barrier, len(plane) + len(column) - 1)

    def low_copy(k, t, source, target):
        along, across = lax.rem(fast + t, SIDE), lax.rem(slow + t, SIDE)
        if k == 0:
            ty, tx = jnp.where(core == 0, y, along), jnp.where(core == 0, along, x)
        else:
            ty, tx = jnp.where(core == 0, across, y), jnp.where(core == 0, x, across)
        return pltpu.make_async_remote_copy(
            src_ref=source,
            dst_ref=target,
            send_sem=low_send.at[k * (SIDE - 1) + t - 1],
            recv_sem=low_recv.at[k * (SIDE - 1) + t - 1],
            device_id=device(ty, tx, core),
            device_id_type=MESH,
        )

    own_low = low.at[pl.ds(pl.multiple_of(z * PIECE, PIECE), PIECE), :]
    own_line = lows.at[z, core, slow]
    low_first = [low_copy(0, t, own_low, lows.at[z, core, slow, fast]) for t in range(1, SIDE)]
    low_then = [low_copy(1, t, own_line, own_line) for t in range(1, SIDE)]
    low_copies = low_first + low_then
    for c in low_first:
        c.start()
    nz_copies = [
        pltpu.make_async_remote_copy(
            src_ref=norm_own.at[0],
            dst_ref=norm_z.at[z],
            send_sem=nz_send.at[dz - 1],
            recv_sem=nz_recv.at[dz - 1],
            device_id=device(y, x, core, lax.rem(z + dz, SIDE)),
            device_id_type=MESH,
        )
        for dz in range(1, SIDE)
    ]

    def row_copy(i, hop):
        ty, tx, tc = at(by_core(core, hop[0]), by_core(core, hop[1]), hop[2])
        to = (ty * SIDE + tx) * CORES + tc
        return pltpu.make_async_remote_copy(
            src_ref=w.at[:, pl.ds(pl.multiple_of(to * COLS, 128), COLS)],
            dst_ref=rows.at[pl.ds(pl.multiple_of(me * ROWS, ROWS), ROWS), :],
            send_sem=send.at[i],
            recv_sem=recv.at[i],
            device_id=device(ty, tx, tc),
            device_id_type=MESH,
        )

    copies = [[row_copy(FIRST[k] + i, hop) for i, hop in enumerate(s)] for k, s in enumerate(STAGES)]

    def start(k):
        if k >= AHEAD:
            for c in copies[k - AHEAD]:
                c.wait_send()
        for c in copies[k]:
            c.start()

    def add_block(source_chip, source_core):
        base = (source_chip * CORES + source_core) * ROWS
        sy, sx = source_chip // SIDE, lax.rem(source_chip, SIDE)
        line, place = jnp.where(source_core == 0, sy, sx), jnp.where(source_core == 0, sx, sy)
        for r in range(0, ROWS, STEP):
            left = lows[:, source_core, line, place, :, r : r + STEP].reshape(RANK, STEP)
            change = lax.dot_general(
                left, own_high[...], (((0,), (0,)), ((), ())), preferred_element_type=jnp.float32
            )
            fresh = rows[pl.ds(pl.multiple_of(base + r, STEP), STEP), :].astype(jnp.float32) + change
            fresh_out[pl.ds(pl.multiple_of(base + r, STEP), STEP), :] = fresh
            total[...] += jnp.abs(fresh).reshape(STEP // 8, 8, COLS).sum(axis=0)

    def take(k):
        stage = STAGES[k]

        def one(i, carry):
            def pick(values):
                out = values[0]
                for j in range(1, len(values)):
                    out = jnp.where(i == j, values[j], out)
                return out

            dc = pick([h[2] for h in stage])
            source_core = lax.rem(core + dc, CORES)
            dy = jnp.where(source_core == 0, pick([h[0][0] for h in stage]), pick([h[0][1] for h in stage]))
            dx = jnp.where(source_core == 0, pick([h[1][0] for h in stage]), pick([h[1][1] for h in stage]))
            source_chip = lax.rem(y + SIDE - dy, SIDE) * SIDE + lax.rem(x + SIDE - dx, SIDE)
            base = (source_chip * CORES + source_core) * ROWS
            landed = rows.at[pl.ds(pl.multiple_of(base, ROWS), ROWS), :]
            pltpu.make_async_copy(landed, landed, recv.at[FIRST[k] + i]).wait()
            add_block(source_chip, source_core)
            return carry

        lax.fori_loop(0, len(stage), one, 0)

    start(0)
    start(1)

    for c in get_norms:
        c.wait()
    norm_own[0, :, 0:NORM] = (norm_in[0] + norm_in[1]).astype(jnp.bfloat16).astype(jnp.float32)
    for c in nz_copies:
        c.start()
    norm_z[z] = norm_own[0]
    for c in nz_copies:
        c.wait_recv()
    lane = lax.broadcasted_iota(jnp.int32, (1, 128), 1)
    second = pltpu.roll(norm_z[1], NORM, 1)
    third = pltpu.roll(norm_z[2], 64, 1)
    fourth = pltpu.roll(norm_z[3], 32, 1)
    norm_mid[0] = jnp.where(lane < NORM, norm_z[0], second)
    norm_mid[1] = jnp.where(lane < 64, second, third)
    norm_mid[2] = jnp.where(lane < 32, third, fourth)
    norm_all[core, y, x] = norm_mid[...]
    own_high[...] = own_high_half(get_high, own_high)
    total[...] = jnp.zeros_like(total)

    start(2)
    def norm_copy(k, source, target, to):
        return pltpu.make_async_remote_copy(
            src_ref=source,
            dst_ref=target,
            send_sem=n_send.at[k],
            recv_sem=n_recv.at[k],
            device_id=to,
            device_id_type=MESH,
        )

    norm_x = [
        norm_copy(t - 1, norm_mid, norm_all.at[core, y, x], device(*at(0, t, 0))) for t in range(1, SIDE)
    ]
    norm_y = [
        norm_copy(t + 2, norm_all.at[core, y], norm_all.at[core, y], device(*at(t, 0, 0)))
        for t in range(1, SIDE)
    ]
    norm_c = [norm_copy(6, norm_all.at[core], norm_all.at[core], device(*at(0, 0, 1)))]
    norm_copies = norm_x + norm_y + norm_c
    low_zcopies = []
    for k, (dz, dc) in enumerate(column):
        low_zcopies.append(
            pltpu.make_async_remote_copy(
                src_ref=lows.at[z, core],
                dst_ref=lows.at[z, core],
                send_sem=low_zsend.at[k],
                recv_sem=low_zrecv.at[k],
                device_id=device(y, x, lax.rem(core + dc, CORES), lax.rem(z + dz, SIDE)),
                device_id_type=MESH,
            )
        )
    start(3)
    get_low.wait()
    for c in low_first:
        c.wait_recv()
    for c in low_then + norm_x:
        c.start()
    start(4)
    start(5)
    for c in low_then + norm_x:
        c.wait_recv()
    for c in low_zcopies + norm_y:
        c.start()
    start(6)
    for c in low_zcopies:
        c.wait_recv()
    get_rows.wait()
    add_block(chip, core)
    take(0)
    take(1)
    take(2)
    take(3)
    take(4)
    for c in norm_y:
        c.wait_recv()
    for c in norm_c:
        c.start()
    take(5)
    for c in norm_c:
        c.wait_recv()
    for c in range(CORES):
        for n in range(CHIPS):
            k = (n * CORES + c) * 3
            norms[k : k + 3] = norm_all[c, n // SIDE, n % SIDE]
    take(6)
    for k in range(len(STAGES) - AHEAD, len(STAGES)):
        for c in copies[k]:
            c.wait_send()
    for c in low_copies + low_zcopies + nz_copies + norm_copies:
        c.wait_send()
    scale[...] = total[...].sum(axis=0, keepdims=True) / D_MODEL


def own_high_half(copy, own_high):
    copy.wait()
    return (own_high[...].astype(jnp.float32) * mix_rate).astype(jnp.bfloat16)


SLOTS = 8


def finish(fresh, scale, norms, serve, scale_out, norm_out, slots, sems, scale_row, norm_rows, small):
    inverse = jnp.broadcast_to(1.0 / scale[...], (8, COLS))

    def put(n, slot):
        to = serve.at[pl.ds(pl.multiple_of(n * ROWS, ROWS), ROWS), :]
        return pltpu.make_async_copy(slots.at[slot], to, sems.at[slot])

    def one(n, carry):
        slot = lax.rem(n, SLOTS)

        @pl.when(n >= SLOTS)
        def _():
            put(n - SLOTS, slot).wait()

        part = fresh[pl.ds(pl.multiple_of(n * ROWS, ROWS), ROWS), :].reshape(ROWS // 8, 8, COLS)
        slots[slot] = (part * inverse).reshape(ROWS, COLS).astype(jnp.bfloat16)
        put(n, slot).start()
        return carry

    lax.fori_loop(0, GROUP - SLOTS, one, 0)
    scale_row[...] = scale[...].reshape(COLS)
    norm_rows[...] = norms[...].reshape(D_MODEL // 128, 128).astype(jnp.bfloat16)
    rest = [
        pltpu.make_async_copy(scale_row, scale_out, small.at[0]),
        pltpu.make_async_copy(norm_rows, norm_out, small.at[1]),
    ]
    for c in rest:
        c.start()
    lax.fori_loop(GROUP - SLOTS, GROUP, one, 0)
    for c in rest:
        c.wait()
    for n in range(GROUP - SLOTS, GROUP):
        put(n, n % SLOTS).wait()


def per_device(w_up, low_up, high_up, norm_train, norm_step):
    dma = pltpu.SemaphoreType.DMA
    vmem = pl.BlockSpec(memory_space=pltpu.VMEM)
    column = SIDE * CORES - 1
    total = FIRST[-1]
    operands = (w_up, low_up.T, high_up, norm_train.reshape(1, NORM), norm_step.reshape(1, NORM))
    gathered = pl.pallas_call(
        exchange,
        out_shape=(
            pltpu.VMEM((D_MODEL, COLS), jnp.float32),
            pltpu.VMEM((1, COLS), jnp.float32),
            pltpu.VMEM((D_MODEL // 128, 1, 128), jnp.float32),
        ),
        in_specs=[pl.BlockSpec(memory_space=pltpu.HBM)] * 5,
        out_specs=(vmem,) * 3,
        scratch_shapes=[
            pltpu.VMEM((D_MODEL, COLS), jnp.bfloat16),
            pltpu.VMEM((SIDE, CORES, SIDE, SIDE, PIECE, ROWS), jnp.bfloat16),
            pltpu.VMEM((RANK, COLS), jnp.bfloat16),
            pltpu.VMEM((2, 1, NORM), jnp.float32),
            pltpu.VMEM((1, 1, 128), jnp.float32),
            pltpu.VMEM((SIDE, 1, 128), jnp.float32),
            pltpu.VMEM((3, 1, 128), jnp.float32),
            pltpu.VMEM((CORES, SIDE, SIDE, 3, 1, 128), jnp.float32),
            pltpu.VMEM((8, COLS), jnp.float32),
            dma((total,)),
            dma((total,)),
            dma((2 * (SIDE - 1),)),
            dma((2 * (SIDE - 1),)),
            dma((column,)),
            dma((column,)),
            dma((SIDE - 1,)),
            dma((SIDE - 1,)),
            dma((2 * SIDE - 1,)),
            dma((2 * SIDE - 1,)),
            dma((5,)),
        ],
        compiler_params=pltpu.CompilerParams(
            collective_id=0, has_side_effects=True, vmem_limit_bytes=20 * 2**20
        ),
        name="exchange",
    )(*(pltpu.with_memory_space_constraint(a, pltpu.HBM) for a in operands))
    serve_up, scale_up, serve_norm = pl.pallas_call(
        finish,
        out_shape=(
            jax.ShapeDtypeStruct((D_MODEL, COLS), jnp.bfloat16),
            jax.ShapeDtypeStruct((COLS,), jnp.float32),
            jax.ShapeDtypeStruct((D_MODEL // 128, 128), jnp.bfloat16),
        ),
        in_specs=[vmem] * 3,
        out_specs=(pl.BlockSpec(memory_space=pltpu.HBM),) * 3,
        scratch_shapes=[
            pltpu.VMEM((SLOTS, ROWS, COLS), jnp.bfloat16),
            dma((SLOTS,)),
            pltpu.VMEM((COLS,), jnp.float32),
            pltpu.VMEM((D_MODEL // 128, 128), jnp.bfloat16),
            dma((2,)),
        ],
        compiler_params=pltpu.CompilerParams(vmem_limit_bytes=6 * 2**20),
        name="finish",
    )(*gathered)
    return serve_up, scale_up, serve_norm.reshape(D_MODEL)


def solution(mesh):
    torus = Mesh(
        mesh.devices.reshape(SIDE, SIDE, CORES, mesh.shape["width"]),
        ("shard_0", "shard_1", "shard_2", "width"),
    )
    in_specs = (P(SHARD, "width"), P(SHARD, None), P(None, "width"), P(SHARD_WIDTH), P(SHARD_WIDTH))
    out_specs = (P(None, WIDTH_SHARD), P(WIDTH_SHARD), P())
    return jax.shard_map(
        per_device, mesh=torus, in_specs=in_specs, out_specs=out_specs, check_vma=False
    )
```

```python
import functools

import jax
import jax.numpy as jnp
from jax import lax
from jax.experimental import pallas as pl
from jax.experimental.pallas import tpu as pltpu
from jax.sharding import Mesh
from jax.sharding import PartitionSpec as P

D_MODEL = 12288
RANK = 64
SIDE = 4
CORES = 2
CHIPS = SIDE * SIDE
GROUP = CHIPS * CORES
ROWS = D_MODEL // GROUP
COLS = 384
PIECE = RANK // SIDE
NORM = 96
STEP = 128
SHARD = ("shard_0", "shard_1", "shard_2")
SHARD_WIDTH = ("shard_0", "shard_1", "shard_2", "width")
WIDTH_SHARD = ("width", "shard_0", "shard_1", "shard_2")
MESH = pl.DeviceIdType.MESH

mix_rate = 0.5


def hops(*pairs):
    def wrapped(v):
        return tuple(q % SIDE for q in v) if isinstance(v, tuple) else (v % SIDE,) * 2

    return [(wrapped(dy), wrapped(dx), dc) for dc in range(CORES) for dy, dx in pairs]


STAGES = [
    hops((1, 1), (-1, -1)) + [((0, 0), (0, 0), 1)],
    hops((1, -1), (-1, 1)),
    hops((2, 2)),
    hops((0, 2), (2, 0)),
    hops((1, 0), (-1, 0), (1, 2), (-1, 2)),
    hops(((2, 0), 1), ((2, 0), -1)),
    hops(((0, 2), 1), ((0, 2), -1)),
]
FIRST = [sum(len(s) for s in STAGES[:k]) for k in range(len(STAGES) + 1)]
AHEAD = 2


def by_core(core, value):
    return value[0] if value[0] == value[1] else jnp.where(core == 0, value[0], value[1])


def exchange(
    w, low, high, train, step,
    fresh_out, scale, norms,
    rows, lows, own_high, norm_in, norm_own, norm_z, norm_mid, norm_all, total,
    send, recv, low_send, low_recv, low_zsend, low_zrecv, nz_send, nz_recv, n_send, n_recv, local,
):
    y, x, core = (lax.axis_index(a) for a in SHARD)
    z = lax.axis_index("width")
    chip = y * SIDE + x
    me = chip * CORES + core
    slow, fast = jnp.where(core == 0, y, x), jnp.where(core == 0, x, y)

    def at(dy, dx, dc):
        return lax.rem(y + dy, SIDE), lax.rem(x + dx, SIDE), lax.rem(core + dc, CORES)

    def device(ty, tx, tc, tz=None):
        return {"shard_0": ty, "shard_1": tx, "shard_2": tc, "width": z if tz is None else tz}

    plane = [(dy, dx, dc) for dy in range(SIDE) for dx in range(SIDE) for dc in range(CORES)][1:]
    column = [(dz, dc) for dz in range(SIDE) for dc in range(CORES)][1:]

    barrier = pltpu.get_barrier_semaphore()
    for dy, dx, dc in plane:
        pl.semaphore_signal(barrier, inc=1, device_id=device(*at(dy, dx, dc)), device_id_type=MESH)
    for dz, dc in column[1:]:
        to = device(y, x, lax.rem(core + dc, CORES), lax.rem(z + dz, SIDE))
        pl.semaphore_signal(barrier, inc=1, device_id=to, device_id_type=MESH)
    get_high = pltpu.make_async_copy(
        high.at[:, pl.ds(pl.multiple_of(me * COLS, 128), COLS)], own_high, local.at[0]
    )
    get_high.start()
    get_rows = pltpu.make_async_copy(
        w.at[:, pl.ds(pl.multiple_of(me * COLS, 128), COLS)],
        rows.at[pl.ds(pl.multiple_of(me * ROWS, ROWS), ROWS), :],
        local.at[1],
    )
    get_rows.start()
    get_low = pltpu.make_async_copy(
        low.at[pl.ds(pl.multiple_of(z * PIECE, PIECE), PIECE), :], lows.at[z, core, slow, fast], local.at[2]
    )
    get_low.start()
    get_norms = [
        pltpu.make_async_copy(part, norm_in.at[k], local.at[3 + k]) for k, part in enumerate((train, step))
    ]
    for c in get_norms:
        c.start()
    norm_own[...] = jnp.zeros_like(norm_own)

    pl.semaphore_wait(barrier, len(plane) + len(column) - 1)

    def low_copy(k, t, source, target):
        along, across = lax.rem(fast + t, SIDE), lax.rem(slow + t, SIDE)
        if k == 0:
            ty, tx = jnp.where(core == 0, y, along), jnp.where(core == 0, along, x)
        else:
            ty, tx = jnp.where(core == 0, across, y), jnp.where(core == 0, x, across)
        return pltpu.make_async_remote_copy(
            src_ref=source,
            dst_ref=target,
            send_sem=low_send.at[k * (SIDE - 1) + t - 1],
            recv_sem=low_recv.at[k * (SIDE - 1) + t - 1],
            device_id=device(ty, tx, core),
            device_id_type=MESH,
        )

    own_low = low.at[pl.ds(pl.multiple_of(z * PIECE, PIECE), PIECE), :]
    own_line = lows.at[z, core, slow]
    low_first = [low_copy(0, t, own_low, lows.at[z, core, slow, fast]) for t in range(1, SIDE)]
    low_then = [low_copy(1, t, own_line, own_line) for t in range(1, SIDE)]
    low_copies = low_first + low_then
    for c in low_first:
        c.start()
    nz_copies = [
        pltpu.make_async_remote_copy(
            src_ref=norm_own.at[0],
            dst_ref=norm_z.at[z],
            send_sem=nz_send.at[dz - 1],
            recv_sem=nz_recv.at[dz - 1],
            device_id=device(y, x, core, lax.rem(z + dz, SIDE)),
            device_id_type=MESH,
        )
        for dz in range(1, SIDE)
    ]

    def row_copy(i, hop):
        ty, tx, tc = at(by_core(core, hop[0]), by_core(core, hop[1]), hop[2])
        to = (ty * SIDE + tx) * CORES + tc
        return pltpu.make_async_remote_copy(
            src_ref=w.at[:, pl.ds(pl.multiple_of(to * COLS, 128), COLS)],
            dst_ref=rows.at[pl.ds(pl.multiple_of(me * ROWS, ROWS), ROWS), :],
            send_sem=send.at[i],
            recv_sem=recv.at[i],
            device_id=device(ty, tx, tc),
            device_id_type=MESH,
        )

    copies = [[row_copy(FIRST[k] + i, hop) for i, hop in enumerate(s)] for k, s in enumerate(STAGES)]

    def start(k):
        if k >= AHEAD:
            for c in copies[k - AHEAD]:
                c.wait_send()
        for c in copies[k]:
            c.start()

    def add_block(source_chip, source_core):
        base = (source_chip * CORES + source_core) * ROWS
        sy, sx = source_chip // SIDE, lax.rem(source_chip, SIDE)
        line, place = jnp.where(source_core == 0, sy, sx), jnp.where(source_core == 0, sx, sy)
        for r in range(0, ROWS, STEP):
            left = lows[:, source_core, line, place, :, r : r + STEP].reshape(RANK, STEP)
            change = lax.dot_general(
                left, own_high[...], (((0,), (0,)), ((), ())), preferred_element_type=jnp.float32
            )
            fresh = rows[pl.ds(pl.multiple_of(base + r, STEP), STEP), :].astype(jnp.float32) + change
            fresh_out[pl.ds(pl.multiple_of(base + r, STEP), STEP), :] = fresh
            total[...] += jnp.abs(fresh).reshape(STEP // 8, 8, COLS).sum(axis=0)

    def take(k):
        stage = STAGES[k]

        def one(i, carry):
            def pick(values):
                out = values[0]
                for j in range(1, len(values)):
                    out = jnp.where(i == j, values[j], out)
                return out

            dc = pick([h[2] for h in stage])
            source_core = lax.rem(core + dc, CORES)
            dy = jnp.where(source_core == 0, pick([h[0][0] for h in stage]), pick([h[0][1] for h in stage]))
            dx = jnp.where(source_core == 0, pick([h[1][0] for h in stage]), pick([h[1][1] for h in stage]))
            source_chip = lax.rem(y + SIDE - dy, SIDE) * SIDE + lax.rem(x + SIDE - dx, SIDE)
            base = (source_chip * CORES + source_core) * ROWS
            landed = rows.at[pl.ds(pl.multiple_of(base, ROWS), ROWS), :]
            pltpu.make_async_copy(landed, landed, recv.at[FIRST[k] + i]).wait()
            add_block(source_chip, source_core)
            return carry

        lax.fori_loop(0, len(stage), one, 0)

    start(0)
    start(1)

    for c in get_norms:
        c.wait()
    norm_own[0, :, 0:NORM] = (norm_in[0] + norm_in[1]).astype(jnp.bfloat16).astype(jnp.float32)
    for c in nz_copies:
        c.start()
    norm_z[z] = norm_own[0]
    for c in nz_copies:
        c.wait_recv()
    lane = lax.broadcasted_iota(jnp.int32, (1, 128), 1)
    second = pltpu.roll(norm_z[1], NORM, 1)
    third = pltpu.roll(norm_z[2], 64, 1)
    fourth = pltpu.roll(norm_z[3], 32, 1)
    norm_mid[0] = jnp.where(lane < NORM, norm_z[0], second)
    norm_mid[1] = jnp.where(lane < 64, second, third)
    norm_mid[2] = jnp.where(lane < 32, third, fourth)
    norm_all[core, y, x] = norm_mid[...]
    own_high[...] = own_high_half(get_high, own_high)
    total[...] = jnp.zeros_like(total)

    start(2)
    def norm_copy(k, source, target, to):
        return pltpu.make_async_remote_copy(
            src_ref=source,
            dst_ref=target,
            send_sem=n_send.at[k],
            recv_sem=n_recv.at[k],
            device_id=to,
            device_id_type=MESH,
        )

    norm_x = [
        norm_copy(t - 1, norm_mid, norm_all.at[core, y, x], device(*at(0, t, 0))) for t in range(1, SIDE)
    ]
    norm_y = [
        norm_copy(t + 2, norm_all.at[core, y], norm_all.at[core, y], device(*at(t, 0, 0)))
        for t in range(1, SIDE)
    ]
    norm_c = [norm_copy(6, norm_all.at[core], norm_all.at[core], device(*at(0, 0, 1)))]
    norm_copies = norm_x + norm_y + norm_c
    low_zcopies = []
    for k, (dz, dc) in enumerate(column):
        low_zcopies.append(
            pltpu.make_async_remote_copy(
                src_ref=lows.at[z, core],
                dst_ref=lows.at[z, core],
                send_sem=low_zsend.at[k],
                recv_sem=low_zrecv.at[k],
                device_id=device(y, x, lax.rem(core + dc, CORES), lax.rem(z + dz, SIDE)),
                device_id_type=MESH,
            )
        )
    start(3)
    get_low.wait()
    for c in low_first:
        c.wait_recv()
    for c in low_then + norm_x:
        c.start()
    start(4)
    start(5)
    for c in low_then + norm_x:
        c.wait_recv()
    for c in low_zcopies + norm_y:
        c.start()
    start(6)
    for c in low_zcopies:
        c.wait_recv()
    get_rows.wait()
    add_block(chip, core)
    take(0)
    take(1)
    take(2)
    take(3)
    take(4)
    for c in norm_y:
        c.wait_recv()
    for c in norm_c:
        c.start()
    take(5)
    for c in norm_c:
        c.wait_recv()
    for c in range(CORES):
        for n in range(CHIPS):
            k = (n * CORES + c) * 3
            norms[k : k + 3] = norm_all[c, n // SIDE, n % SIDE]
    take(6)
    for k in range(len(STAGES) - AHEAD, len(STAGES)):
        for c in copies[k]:
            c.wait_send()
    for c in low_copies + low_zcopies + nz_copies + norm_copies:
        c.wait_send()
    scale[...] = total[...].sum(axis=0, keepdims=True) / D_MODEL


def own_high_half(copy, own_high):
    copy.wait()
    return (own_high[...].astype(jnp.float32) * mix_rate).astype(jnp.bfloat16)


SLOTS = 8


def finish(fresh, scale, norms, serve, scale_out, norm_out, slots, sems, scale_row, norm_rows, small):
    inverse = jnp.broadcast_to(1.0 / scale[...], (8, COLS))

    def put(n, slot):
        to = serve.at[pl.ds(pl.multiple_of(n * ROWS, ROWS), ROWS), :]
        return pltpu.make_async_copy(slots.at[slot], to, sems.at[slot])

    def one(n, carry):
        slot = lax.rem(n, SLOTS)

        @pl.when(n >= SLOTS)
        def _():
            put(n - SLOTS, slot).wait()

        part = fresh[pl.ds(pl.multiple_of(n * ROWS, ROWS), ROWS), :].reshape(ROWS // 8, 8, COLS)
        slots[slot] = (part * inverse).reshape(ROWS, COLS).astype(jnp.bfloat16)
        put(n, slot).start()
        return carry

    lax.fori_loop(0, GROUP - SLOTS, one, 0)
    scale_row[...] = scale[...].reshape(COLS)
    norm_rows[...] = norms[...].reshape(D_MODEL // 128, 128).astype(jnp.bfloat16)
    rest = [
        pltpu.make_async_copy(scale_row, scale_out, small.at[0]),
        pltpu.make_async_copy(norm_rows, norm_out, small.at[1]),
    ]
    for c in rest:
        c.start()
    lax.fori_loop(GROUP - SLOTS, GROUP, one, 0)
    for c in rest:
        c.wait()
    for n in range(GROUP - SLOTS, GROUP):
        put(n, n % SLOTS).wait()


def per_device(w_up, low_up, high_up, norm_train, norm_step):
    dma = pltpu.SemaphoreType.DMA
    vmem = pl.BlockSpec(memory_space=pltpu.VMEM)
    column = SIDE * CORES - 1
    total = FIRST[-1]
    operands = (w_up, low_up.T, high_up, norm_train.reshape(1, NORM), norm_step.reshape(1, NORM))
    gathered = pl.pallas_call(
        exchange,
        out_shape=(
            pltpu.VMEM((D_MODEL, COLS), jnp.float32),
            pltpu.VMEM((1, COLS), jnp.float32),
            pltpu.VMEM((D_MODEL // 128, 1, 128), jnp.float32),
        ),
        in_specs=[pl.BlockSpec(memory_space=pltpu.HBM)] * 5,
        out_specs=(vmem,) * 3,
        scratch_shapes=[
            pltpu.VMEM((D_MODEL, COLS), jnp.bfloat16),
            pltpu.VMEM((SIDE, CORES, SIDE, SIDE, PIECE, ROWS), jnp.bfloat16),
            pltpu.VMEM((RANK, COLS), jnp.bfloat16),
            pltpu.VMEM((2, 1, NORM), jnp.float32),
            pltpu.VMEM((1, 1, 128), jnp.float32),
            pltpu.VMEM((SIDE, 1, 128), jnp.float32),
            pltpu.VMEM((3, 1, 128), jnp.float32),
            pltpu.VMEM((CORES, SIDE, SIDE, 3, 1, 128), jnp.float32),
            pltpu.VMEM((8, COLS), jnp.float32),
            dma((total,)),
            dma((total,)),
            dma((2 * (SIDE - 1),)),
            dma((2 * (SIDE - 1),)),
            dma((column,)),
            dma((column,)),
            dma((SIDE - 1,)),
            dma((SIDE - 1,)),
            dma((2 * SIDE - 1,)),
            dma((2 * SIDE - 1,)),
            dma((5,)),
        ],
        compiler_params=pltpu.CompilerParams(
            collective_id=0, has_side_effects=True, vmem_limit_bytes=20 * 2**20
        ),
        name="exchange",
    )(*(pltpu.with_memory_space_constraint(a, pltpu.HBM) for a in operands))
    serve_up, scale_up, serve_norm = pl.pallas_call(
        finish,
        out_shape=(
            jax.ShapeDtypeStruct((D_MODEL, COLS), jnp.bfloat16),
            jax.ShapeDtypeStruct((COLS,), jnp.float32),
            jax.ShapeDtypeStruct((D_MODEL // 128, 128), jnp.bfloat16),
        ),
        in_specs=[vmem] * 3,
        out_specs=(pl.BlockSpec(memory_space=pltpu.HBM),) * 3,
        scratch_shapes=[
            pltpu.VMEM((SLOTS, ROWS, COLS), jnp.bfloat16),
            dma((SLOTS,)),
            pltpu.VMEM((COLS,), jnp.float32),
            pltpu.VMEM((D_MODEL // 128, 128), jnp.bfloat16),
            dma((2,)),
        ],
        compiler_params=pltpu.CompilerParams(vmem_limit_bytes=6 * 2**20),
        name="finish",
    )(*gathered)
    return serve_up, scale_up, serve_norm.reshape(D_MODEL)


def solution(mesh):
    torus = Mesh(
        mesh.devices.reshape(SIDE, SIDE, CORES, mesh.shape["width"]),
        ("shard_0", "shard_1", "shard_2", "width"),
    )
    in_specs = (P(SHARD, "width"), P(SHARD, None), P(None, "width"), P(SHARD_WIDTH), P(SHARD_WIDTH))
    out_specs = (P(None, WIDTH_SHARD), P(WIDTH_SHARD), P())
    return jax.shard_map(
        per_device, mesh=torus, in_specs=in_specs, out_specs=out_specs, check_vma=False
    )
```
